256 devices in a mesh: unit: 4 (over z_hi), zero: 16 (over y, x), tp: 4 (over z_lo, core).
Axes of the slice: x: 4, y: 4, z: 8 (z_hi: 4, z_lo: 2; z = z_hi * 2 + z_lo), core: 2. Of those that a mesh axis runs over, the one named last changes fastest.
Arguments:
- weight_query: bfloat16 [16384, 4096], P(('unit', 'zero'), 'tp'), parts along dimension 0, may hold values from -0.125 to 0.125
- low_query: bfloat16 [16384, 32], P(('unit', 'zero')), parts along dimension 0, may hold values from -0.09375 to 0.09375
- high_query: bfloat16 [128, 4096], P('unit', 'tp'), parts along dimension 0, may hold values from -1 to 1
- weight_key: bfloat16 [16384, 1024], P(('unit', 'zero'), 'tp'), parts along dimension 0, may hold values from -0.125 to 0.125
- low_key: bfloat16 [16384, 32], P(('unit', 'zero')), parts along dimension 0, may hold values from -0.09375 to 0.09375
- high_key: bfloat16 [128, 1024], P('unit', 'tp'), parts along dimension 0, may hold values from -1 to 1
- weight_value: bfloat16 [16384, 1024], P(('unit', 'zero'), 'tp'), parts along dimension 0, may hold values from -0.125 to 0.125
- low_value: bfloat16 [16384, 32], P(('unit', 'zero')), parts along dimension 0, may hold values from -0.09375 to 0.09375
- high_value: bfloat16 [128, 1024], P('unit', 'tp'), parts along dimension 0, may hold values from -1 to 1
- norm_train: float32 [16384], P(('unit', 'zero', 'tp')), parts along dimension 0, may hold values from 0.25 to 1.75
- norm_step: float32 [16384], P(('unit', 'zero', 'tp')), parts along dimension 0, may hold values from -0.3 to 0.3
Outputs:
- serve_query: bfloat16 [16384, 4096], P('unit', 'tp'), parts along dimension 0
- serve_key: bfloat16 [16384, 1024], P('unit', 'tp'), parts along dimension 0
- serve_value: bfloat16 [16384, 1024], P('unit', 'tp'), parts along dimension 0
- column_query: float32 [16384], P(('unit', 'tp')), parts along dimension 0
- column_key: float32 [4096], P(('unit', 'tp')), parts along dimension 0
- column_value: float32 [4096], P(('unit', 'tp')), parts along dimension 0
- serve_norm: bfloat16 [16384], P('unit'), parts along dimension 0
The draws below stay inside these ranges and needn't reach their ends.
There are 4 independent parts, one for each index of `unit`. The reference program is written for one: setup_inputs(seed, part) draws one part's arguments, and reference() takes and returns one part's arrays. A program takes and returns all parts, laid end to end along the dimension named above; each array names one. Nothing has to cross between parts.
All inputs are finite; a program needn't handle non-finite values.
Results may differ from the reference program's by a relative error of at most 0.001.
Values may be sent and summed in bfloat16 or wider, within the bound.
A program may use at most 64 MiB of HBM per device.

```python
import jax
import jax.numpy as jnp
from jax import lax

D_MODEL = 4096
Q_DIM = 4096
KV_DIM = 1024
RANK = 32


def spiked(drawn, key, source, target, shards_of, factor):
    owner, partner = [(jnp.arange(drawn.shape[dim]) // (drawn.shape[dim] // shards_of)).reshape([-1 if axis == dim else 1 for axis in range(drawn.ndim)]) for dim in (source, target)]
    chosen = jax.random.permutation(key, shards_of)[partner]
    strong = (owner == chosen) | (owner == (partner + shards_of // 2) % shards_of)
    return jnp.where(strong, factor * drawn, drawn)


def block_levels(stream_key, shape, split, smallest, largest):
    loudness = 1.0
    for position, parts in split:
        draws = jax.random.uniform(jax.random.fold_in(jax.random.fold_in(stream_key, 6), position), (parts,), jnp.float32, smallest / len(split), largest / len(split))
        loudness = loudness * jnp.repeat(jnp.exp(draws), shape[position] // parts).reshape((-1,) + (1,) * (len(shape) - 1 - position))
    return loudness


def centred(stream_key, dims, spread, most, pieces=(), kind=jnp.bfloat16):
    entries = jax.random.normal(stream_key, dims, jnp.float32) * spread
    if len(pieces) > 0:
        entries = block_levels(stream_key, dims, pieces, -0.22, 0.18) * entries
    return jnp.clip(entries, min=-most, max=most).astype(kind)


def gaussian_with(rng, extent, scale, reach, shards, heavy, kind=jnp.bfloat16):
    result = scale * jax.random.normal(rng, extent, jnp.float32)
    if shards:
        result = result * block_levels(rng, extent, shards, -0.22, 0.18)
    return jnp.clip(spiked(result, jax.random.fold_in(rng, 3), *heavy), -reach, reach).astype(kind)


def setup_inputs(seed: int = 0, part: int = 0) -> dict:
    streams_of = jax.random.split(jax.random.key(seed), 12)
    part_splits = jax.random.split(jax.random.fold_in(streams_of[11], part), 12)
    weight_query = gaussian_with(part_splits[0], (D_MODEL, Q_DIM), D_MODEL ** -0.5, 0.125, ((0, 16), (1, 4)), (0, 1, 16, 2.0))
    low_query = centred(part_splits[1], (D_MODEL, RANK), D_MODEL ** -0.5, 0.09375, ((0, 16),))
    high_query = centred(part_splits[2], (RANK, Q_DIM), RANK ** -0.5, 1.0, ((1, 4),))
    weight_key = gaussian_with(part_splits[3], (D_MODEL, KV_DIM), D_MODEL ** -0.5, 0.125, ((0, 16), (1, 4)), (0, 1, 16, 2.0))
    low_key = centred(part_splits[4], (D_MODEL, RANK), D_MODEL ** -0.5, 0.09375, ((0, 16),))
    high_key = centred(part_splits[5], (RANK, KV_DIM), RANK ** -0.5, 1.0, ((1, 4),))
    weight_value = gaussian_with(part_splits[6], (D_MODEL, KV_DIM), D_MODEL ** -0.5, 0.125, ((0, 16), (1, 4)), (0, 1, 16, 2.0))
    low_value = centred(part_splits[7], (D_MODEL, RANK), D_MODEL ** -0.5, 0.09375, ((0, 16),))
    high_value = centred(part_splits[8], (RANK, KV_DIM), RANK ** -0.5, 1.0, ((1, 4),))
    norm_train = jnp.clip(1.0 + 0.15 * jax.random.normal(part_splits[9], (D_MODEL,), jnp.float32), 0.25, 1.75)
    norm_step = jnp.clip(jax.random.uniform(part_splits[10], (D_MODEL,), jnp.float32, -0.3, 0.3) * block_levels(part_splits[10], (D_MODEL,), ((0, 64),), -0.4, 0.0), -0.3, 0.3)
    return dict(weight_query=weight_query, low_query=low_query, high_query=high_query, weight_key=weight_key, low_key=low_key, high_key=high_key, weight_value=weight_value, low_value=low_value, high_value=high_value, norm_train=norm_train, norm_step=norm_step)


mix_rate = 2.0

def reference(weight_query, low_query, high_query, weight_key, low_key, high_key, weight_value, low_value, high_value, norm_train, norm_step):
    fresh_query = weight_query.astype(jnp.float32) + mix_rate * jnp.dot(low_query, high_query, preferred_element_type=jnp.float32)
    fresh_key = weight_key.astype(jnp.float32) + mix_rate * jnp.dot(low_key, high_key, preferred_element_type=jnp.float32)
    fresh_value = weight_value.astype(jnp.float32) + mix_rate * jnp.dot(low_value, high_value, preferred_element_type=jnp.float32)
    column_query = jnp.sqrt(lax.optimization_barrier(jnp.sum(fresh_query * fresh_query, axis=0)))
    serve_query = (fresh_query / column_query).astype(jnp.bfloat16)
    column_key = jnp.sqrt(lax.optimization_barrier(jnp.sum(fresh_key * fresh_key, axis=0)))
    serve_key = (fresh_key / column_key).astype(jnp.bfloat16)
    column_value = jnp.sqrt(lax.optimization_barrier(jnp.sum(fresh_value * fresh_value, axis=0)))
    serve_value = (fresh_value / column_value).astype(jnp.bfloat16)
    serve_norm = (norm_train + norm_step).astype(jnp.bfloat16)
    return (serve_query, serve_key, serve_value, column_query, column_key, column_value, serve_norm)
```

```python
import jax
import jax.numpy as jnp
from jax import lax
from jax.experimental import pallas as pl
from jax.experimental.pallas import tpu as pltpu
from jax.sharding import PartitionSpec as P

MESH = pl.DeviceIdType.MESH
SIDE = 4
BLOCKS = SIDE * SIDE
TP = 4
RANK = 32
ROWS = 256
Q, KV = 1024, 256
COLS = Q + 2 * KV
AHEAD = 4
DIRECTIONS = ((0, 1), (0, -1), (1, 1), (1, -1))

BULK = [(0, 1, 1), (0, 1, 1), (0, 1, -1), (0, -1, 1), (0, -1, -1), (0, -1, -1)]
BULK = BULK + [(1, s1, s2) for _, s1, s2 in BULK]
BULK_PLACE = [("q", 0), ("q", 1), ("k", 0), ("q", 2), ("v", 0), ("q", 3)]
BULK_PLACE = BULK_PLACE + [("q", 4), ("q", 5), ("k", 1), ("q", 6), ("v", 1), ("q", 7)]
SMALL = [(0, 1, 1), (1, -1, -1), (1, 1, 1)]


def children(tree, a, b):
    first, far1, far2 = tree
    out = []
    for axis, sign, here, far, along in (
        (first, 1, a, far1, 0),
        (first, -1, a, far1, 0),
        (1 - first, 1, b, far2, 1),
        (1 - first, -1, b, far2, 1),
    ):
        if along == 0 and b != 0:
            continue
        goes = here == 0 or (here == sign % SIDE and far == sign)
        if goes:
            to = (here + sign) % SIDE
            out.append(((axis, sign), (to, b) if along == 0 else (a, to)))
    return out


def depth(tree, a, b):
    return max((1 + depth(tree, *to) for _, to in children(tree, a, b)), default=0)


def offsets(tree, a, b):
    return (b, a) if tree[0] == 0 else (a, b)


def plan(trees, ahead, one_per_step):
    ready = {d: [] for d in DIRECTIONS}

    def offer(c, a, b, at):
        for d, to in children(trees[c], a, b):
            ready[d].append((at, c, a, b, to))

    for c in range(len(trees)):
        offer(c, 0, 0, -ahead)
    steps = []
    while any(ready.values()):
        s = len(steps)
        now = {}
        for d in DIRECTIONS:
            can = [r for r in ready[d] if r[0] <= s - ahead]
            can.sort(key=lambda r: (-depth(trees[r[1]], *r[4]), r[0], r[1]))
            now[d] = can[:1] if one_per_step else can
            for r in now[d]:
                ready[d].remove(r)
        for d in DIRECTIONS:
            for _, c, a, b, to in now[d]:
                offer(c, *to, s)
        steps.append({d: [r[1:] for r in now[d]] for d in DIRECTIONS})
    return steps


STEPS = plan(BULK, AHEAD, True)
SMALL_STEPS = plan(SMALL, AHEAD, False)
N = len(STEPS)


def gather_kernel(
    wq, wk, wv, lq, lk, lv, hq, hk, hv, train, step_in,
    rq, rk, rv, low, sums, norms,
    load_sem, send_sem, recv_sem, small_send, small_recv, tp_send, tp_recv,
):
    me = lax.axis_index("zero")
    t = lax.axis_index("tp")
    y, x = me // SIDE, me % SIDE

    def block(dy, dx):
        return ((y + SIDE - dy) % SIDE) * SIDE + (x + SIDE - dx) % SIDE

    blk = {(dy, dx): block(dy, dx) for dy in range(SIDE) for dx in range(SIDE)}
    towards = {
        (axis, sign): blk[(0, -sign % SIDE) if axis == 0 else (-sign % SIDE, 0)]
        for axis, sign in DIRECTIONS
    }

    barrier = pltpu.get_barrier_semaphore()
    for d in DIRECTIONS:
        pl.semaphore_signal(barrier, inc=1, device_id={"zero": towards[d]}, device_id_type=MESH)
    for i in range(1, TP):
        pl.semaphore_signal(barrier, inc=1, device_id={"tp": (t + i) % TP}, device_id_type=MESH)

    loads = [
        pltpu.make_async_copy(src, dst.at[me], load_sem.at[i])
        for i, (src, dst) in enumerate(((wq, rq), (wk, rk), (wv, rv)))
    ]
    for load in loads:
        load.start()

    @pl.when(t == 0)
    def _():
        low[t, me] = lq[...]

    @pl.when(t == 1)
    def _():
        low[t, me] = lk[...]

    @pl.when(t >= 2)
    def _():
        low[t, me] = lv[...]

    for load in loads:
        load.wait()
    pl.semaphore_wait(barrier, len(DIRECTIONS) + TP - 1)

    def bulk_ref(c, a, b):
        which, i = BULK_PLACE[c]
        ref = {"q": rq, "k": rk, "v": rv}[which]
        rows = 32 if which == "q" else 128
        return ref.at[blk[offsets(BULK[c], a, b)], pl.ds(rows * i, rows)]

    def bulk_copy(s, k, opposite):
        d = DIRECTIONS[k]
        c, a, b, to = STEPS[s][d][0]
        ref = bulk_ref(c, *(to if opposite else (a, b)))
        return pltpu.make_async_remote_copy(
            src_ref=ref, dst_ref=ref, send_sem=send_sem.at[k, s], recv_sem=recv_sem.at[k, s],
            device_id={"zero": towards[d]}, device_id_type=MESH,
        )

    def small_copy(c, a, b, to, d, opposite):
        where = blk[offsets(SMALL[c], *(to if opposite else (a, b)))]
        ref = sums.at[where] if c == 2 else low.at[t, where, pl.ds(16 * c, 16)]
        slot = to[0] * SIDE + to[1]
        return pltpu.make_async_remote_copy(
            src_ref=ref, dst_ref=ref, send_sem=small_send.at[c, slot], recv_sem=small_recv.at[c, slot],
            device_id={"zero": towards[d]}, device_id_type=MESH,
        )

    def smalls(s):
        if 0 <= s < len(SMALL_STEPS):
            for d in DIRECTIONS:
                for c, a, b, to in SMALL_STEPS[s][d]:
                    yield (c, a, b, to, d)

    def sends(s):
        for k, d in enumerate(DIRECTIONS):
            if s < N and STEPS[s][d]:
                bulk_copy(s, k, False).start()

    def receives(s):
        for k, d in enumerate(DIRECTIONS):
            if 0 <= s < N and STEPS[s][d]:
                bulk_copy(s, k, True).wait_recv()

    for s in range(AHEAD):
        sends(s)

    for w, lo, hi, start in ((rq, lq, hq, 0), (rk, lk, hk, Q), (rv, lv, hv, Q + KV)):
        left = lo[...]
        for j in range(w.shape[2] // KV):
            cols = pl.ds(KV * j, KV)
            fresh = w[me, :, cols].astype(jnp.float32) + 2.0 * lax.dot_general(
                left, hi[:, cols], (((0,), (0,)), ((), ())), preferred_element_type=jnp.float32
            )
            sums[me, :, pl.ds(start + KV * j, KV)] = jnp.sum(fresh * fresh, axis=0, keepdims=True)
    sums[me, :, pl.ds(COLS, 128)] = jnp.concatenate([train[...] + step_in[...]] * 2, axis=1)

    lag = AHEAD + 1
    last_small = len(SMALL_STEPS) - 1 + lag
    for s in range(AHEAD, N + AHEAD):
        receives(s - AHEAD)
        for item in smalls(s - lag - AHEAD):
            small_copy(*item, True).wait_recv()
        sends(s)
        for item in smalls(s - lag):
            small_copy(*item, False).start()
        if s == last_small + AHEAD:
            for i in range(1, TP):
                for copy in tp_copies(low, sums, norms, t, t, i, tp_send, tp_recv):
                    copy.start()
    for i in range(1, TP):
        for copy in tp_copies(low, sums, norms, t, (t + TP - i) % TP, i, tp_send, tp_recv):
            copy.wait_recv()
    norms[t] = sums[:, 0, pl.ds(COLS, 128)]
    for i in range(1, TP):
        for copy in tp_copies(low, sums, norms, t, t, i, tp_send, tp_recv):
            copy.wait_send()
    for s in range(len(SMALL_STEPS)):
        for item in smalls(s):
            small_copy(*item, False).wait_send()
    for s in range(N):
        for k, d in enumerate(DIRECTIONS):
            if STEPS[s][d]:
                bulk_copy(s, k, False).wait_send()


def tp_copies(low, sums, norms, t, owner, i, send_sem, recv_sem):
    for j, (src, dst) in enumerate(
        ((low.at[owner], low.at[owner]), (sums.at[:, 0, pl.ds(COLS, 128)], norms.at[owner]))
    ):
        yield pltpu.make_async_remote_copy(
            src_ref=src, dst_ref=dst, send_sem=send_sem.at[i, j], recv_sem=recv_sem.at[i, j],
            device_id={"tp": (t + i) % TP}, device_id_type=MESH,
        )


SLOTS = 4


def merge_kernel(
    rq, rk, rv, low, sums, norms, hq, hk, hv,
    sq, sk, sv, cq, ck, cv, norm_out,
    inv, oq, ok, ov, lines, out_sem,
):
    total = sums[0, :, pl.ds(0, COLS)]
    for b in range(1, BLOCKS):
        total = total + sums[b, :, pl.ds(0, COLS)]
    column = jnp.sqrt(total)
    cq[...] = column[:, :Q]
    ck[...] = column[:, Q : Q + KV]
    cv[...] = column[:, Q + KV :]
    inv[...] = 1.0 / column

    lane = lax.broadcasted_iota(jnp.int32, (BLOCKS, 128), 1)
    for p in range(2):
        lines[pl.ds(p, BLOCKS, stride=2), :] = jnp.where(lane < 64, norms[2 * p], norms[2 * p + 1])
    norm_out[...] = lines[...].astype(jnp.bfloat16)

    parts = ((rq, 0, hq, oq, sq, 0), (rk, 1, hk, ok, sk, Q), (rv, 2, hv, ov, sv, Q + KV))

    def outs(b, slot):
        return [
            pltpu.make_async_copy(o.at[slot], serve.at[pl.ds(b * ROWS, ROWS)], out_sem.at[i, slot])
            for i, (_, _, _, o, serve, _) in enumerate(parts)
        ]

    def one(b, _):
        slot = b % SLOTS

        @pl.when(b >= SLOTS)
        def _():
            for copy in outs(b - SLOTS, slot):
                copy.wait()

        for w, which, hi, o, _, start in parts:
            left = low[which, b]
            for j in range(w.shape[2] // KV):
                cols = pl.ds(KV * j, KV)
                fresh = w[b, :, cols].astype(jnp.float32) + lax.dot_general(
                    left, 2.0 * hi[:, cols], (((0,), (0,)), ((), ())), preferred_element_type=jnp.float32
                )
                o[slot, :, cols] = (fresh * inv[:, pl.ds(start + KV * j, KV)]).astype(jnp.bfloat16)
        for copy in outs(b, slot):
            copy.start()
        return 0

    lax.fori_loop(0, BLOCKS, one, 0)
    for b in range(BLOCKS - SLOTS, BLOCKS):
        for copy in outs(b, b % SLOTS):
            copy.wait()


def on_device(
    weight_query, low_query, high_query,
    weight_key, low_key, high_key,
    weight_value, low_value, high_value,
    norm_train, norm_step,
):
    f32, bf16 = jnp.float32, jnp.bfloat16
    vmem = pl.BlockSpec(memory_space=pltpu.VMEM)
    hbm = pl.BlockSpec(memory_space=pl.ANY)
    highs = (high_query, high_key, high_value)
    dma = pltpu.SemaphoreType.DMA
    gathered = pl.pallas_call(
        gather_kernel,
        name="gather",
        out_shape=(
            pltpu.VMEM((BLOCKS, ROWS, Q), bf16),
            pltpu.VMEM((BLOCKS, ROWS, KV), bf16),
            pltpu.VMEM((BLOCKS, ROWS, KV), bf16),
            pltpu.VMEM((TP, BLOCKS, RANK, ROWS), bf16),
            pltpu.VMEM((BLOCKS, 1, COLS + 128), f32),
            pltpu.VMEM((TP, BLOCKS, 128), f32),
        ),
        in_specs=[hbm] * 3 + [vmem] * 8,
        out_specs=[vmem] * 6,
        scratch_shapes=[
            dma((3,)), dma((4, N)), dma((4, N)), dma((3, BLOCKS)), dma((3, BLOCKS)), dma((TP, 2)), dma((TP, 2)),
        ],
        compiler_params=pltpu.CompilerParams(collective_id=0, has_side_effects=True, vmem_limit_bytes=16 << 20),
    )(
        weight_query, weight_key, weight_value, low_query.T, low_key.T, low_value.T, *highs,
        norm_train.reshape(1, 64), norm_step.reshape(1, 64),
    )
    sq, sk, sv, cq, ck, cv, norm = pl.pallas_call(
        merge_kernel,
        name="merge",
        out_shape=(
            jax.ShapeDtypeStruct((BLOCKS * ROWS, Q), bf16),
            jax.ShapeDtypeStruct((BLOCKS * ROWS, KV), bf16),
            jax.ShapeDtypeStruct((BLOCKS * ROWS, KV), bf16),
            jax.ShapeDtypeStruct((1, Q), f32),
            jax.ShapeDtypeStruct((1, KV), f32),
            jax.ShapeDtypeStruct((1, KV), f32),
            jax.ShapeDtypeStruct((32, 128), bf16),
        ),
        in_specs=[vmem] * 9,
        out_specs=[hbm] * 3 + [vmem] * 4,
        scratch_shapes=[
            pltpu.VMEM((1, COLS), f32),
            pltpu.VMEM((SLOTS, ROWS, Q), bf16),
            pltpu.VMEM((SLOTS, ROWS, KV), bf16),
            pltpu.VMEM((SLOTS, ROWS, KV), bf16),
            pltpu.VMEM((2 * BLOCKS, 128), f32),
            dma((3, SLOTS)),
        ],
        compiler_params=pltpu.CompilerParams(vmem_limit_bytes=24 << 20),
    )(*gathered, *highs)
    return sq, sk, sv, cq.reshape(Q), ck.reshape(KV), cv.reshape(KV), norm.reshape(4096)


def solution(mesh):
    rows = P(("unit", "zero"), "tp")
    low = P(("unit", "zero"), None)
    high = P("unit", "tp")
    norm = P(("unit", "zero", "tp"))
    return jax.shard_map(
        on_device,
        mesh=mesh,
        in_specs=(rows, low, high) * 3 + (norm, norm),
        out_specs=(high, high, high, P(("unit", "tp")), P(("unit", "tp")), P(("unit", "tp")), P("unit")),
        check_vma=False,
    )
```

```python
import jax
import jax.numpy as jnp
from jax import lax
from jax.experimental import pallas as pl
from jax.experimental.pallas import tpu as pltpu
from jax.sharding import PartitionSpec as P

MESH = pl.DeviceIdType.MESH
SIDE = 4
BLOCKS = SIDE * SIDE
TP = 4
RANK = 32
ROWS = 256
Q, KV = 1024, 256
COLS = Q + 2 * KV
AHEAD = 4
TP_WAIT = 10
DIRECTIONS = ((0, 1), (0, -1), (1, 1), (1, -1))

BULK = [(0, 1, 1), (0, 1, 1), (0, 1, -1), (0, -1, 1), (0, -1, -1), (0, -1, -1)]
BULK = BULK + [(1, s1, s2) for _, s1, s2 in BULK]
BULK_PLACE = [("q", 0), ("q", 1), ("k", 0), ("q", 2), ("v", 0), ("q", 3)]
BULK_PLACE = BULK_PLACE + [("q", 4), ("q", 5), ("k", 1), ("q", 6), ("v", 1), ("q", 7)]
SMALL = [(0, 1, 1), (1, -1, -1), (1, 1, 1)]


def children(tree, a, b):
    first, far1, far2 = tree
    out = []
    for axis, sign, here, far, along in (
        (first, 1, a, far1, 0),
        (first, -1, a, far1, 0),
        (1 - first, 1, b, far2, 1),
        (1 - first, -1, b, far2, 1),
    ):
        if along == 0 and b != 0:
            continue
        goes = here == 0 or (here == sign % SIDE and far == sign)
        if goes:
            to = (here + sign) % SIDE
            out.append(((axis, sign), (to, b) if along == 0 else (a, to)))
    return out


def depth(tree, a, b):
    return max((1 + depth(tree, *to) for _, to in children(tree, a, b)), default=0)


def offsets(tree, a, b):
    return (b, a) if tree[0] == 0 else (a, b)


def plan(trees, ahead, one_per_step):
    ready = {d: [] for d in DIRECTIONS}

    def offer(c, a, b, at):
        for d, to in children(trees[c], a, b):
            ready[d].append((at, c, a, b, to))

    for c in range(len(trees)):
        offer(c, 0, 0, -ahead)
    steps = []
    while any(ready.values()):
        s = len(steps)
        now = {}
        for d in DIRECTIONS:
            can = [r for r in ready[d] if r[0] <= s - ahead]
            can.sort(key=lambda r: (-depth(trees[r[1]], *r[4]), r[0], r[1]))
            now[d] = can[:1] if one_per_step else can
            for r in now[d]:
                ready[d].remove(r)
        for d in DIRECTIONS:
            for _, c, a, b, to in now[d]:
                offer(c, *to, s)
        steps.append({d: [r[1:] for r in now[d]] for d in DIRECTIONS})
    return steps


STEPS = plan(BULK, AHEAD, True)
SMALL_STEPS = plan(SMALL, AHEAD, False)
N = len(STEPS)


def gather_kernel(
    wq, wk, wv, lq, lk, lv, hq, hk, hv, train, step_in,
    rq, rk, rv, left, high2, inv, column, norm_out,
    own_low, high, norm_in, low, sums, norms, lines,
    load_sem, send_sem, recv_sem, small_send, small_recv, tp_send, tp_recv,
):
    me = lax.axis_index("zero")
    t = lax.axis_index("tp")
    y, x = me // SIDE, me % SIDE

    def block(dy, dx):
        return ((y + SIDE - dy) % SIDE) * SIDE + (x + SIDE - dx) % SIDE

    blk = {(dy, dx): block(dy, dx) for dy in range(SIDE) for dx in range(SIDE)}
    towards = {
        (axis, sign): blk[(0, -sign % SIDE) if axis == 0 else (-sign % SIDE, 0)]
        for axis, sign in DIRECTIONS
    }

    barrier = pltpu.get_barrier_semaphore()
    for d in DIRECTIONS:
        pl.semaphore_signal(barrier, inc=1, device_id={"zero": towards[d]}, device_id_type=MESH)
    for i in range(1, TP):
        pl.semaphore_signal(barrier, inc=1, device_id={"tp": (t + i) % TP}, device_id_type=MESH)

    loads = [
        pltpu.make_async_copy(src, dst, load_sem.at[i])
        for i, (src, dst) in enumerate(
            (
                (wq, rq.at[me]), (wk, rk.at[me]), (wv, rv.at[me]),
                (lq, own_low.at[0]), (lk, own_low.at[1]), (lv, own_low.at[2]),
                (hq, high.at[:, pl.ds(0, Q)]), (hk, high.at[:, pl.ds(Q, KV)]), (hv, high.at[:, pl.ds(Q + KV, KV)]),
                (train, norm_in.at[0]), (step_in, norm_in.at[1]),
            )
        )
    ]
    for load in loads:
        load.start()
    for load in loads[:3]:
        load.wait()
    pl.semaphore_wait(barrier, len(DIRECTIONS) + TP - 1)

    def bulk_ref(c, a, b):
        which, i = BULK_PLACE[c]
        ref = {"q": rq, "k": rk, "v": rv}[which]
        rows = 32 if which == "q" else 128
        return ref.at[blk[offsets(BULK[c], a, b)], pl.ds(rows * i, rows)]

    def bulk_copy(s, k, opposite):
        d = DIRECTIONS[k]
        c, a, b, to = STEPS[s][d][0]
        ref = bulk_ref(c, *(to if opposite else (a, b)))
        return pltpu.make_async_remote_copy(
            src_ref=ref, dst_ref=ref, send_sem=send_sem.at[k, s], recv_sem=recv_sem.at[k, s],
            device_id={"zero": towards[d]}, device_id_type=MESH,
        )

    def small_copy(c, a, b, to, d, opposite):
        where = blk[offsets(SMALL[c], *(to if opposite else (a, b)))]
        ref = sums.at[where] if c == 2 else low.at[t, where, pl.ds(16 * c, 16)]
        slot = to[0] * SIDE + to[1]
        return pltpu.make_async_remote_copy(
            src_ref=ref, dst_ref=ref, send_sem=small_send.at[c, slot], recv_sem=small_recv.at[c, slot],
            device_id={"zero": towards[d]}, device_id_type=MESH,
        )

    def smalls(s):
        if 0 <= s < len(SMALL_STEPS):
            for d in DIRECTIONS:
                for c, a, b, to in SMALL_STEPS[s][d]:
                    yield (c, a, b, to, d)

    def tp_copies(owner, i):
        for j, (src, dst) in enumerate(
            ((low.at[owner], low.at[owner]), (sums.at[:, 0, pl.ds(COLS, 128)], norms.at[owner]))
        ):
            yield pltpu.make_async_remote_copy(
                src_ref=src, dst_ref=dst, send_sem=tp_send.at[i, j], recv_sem=tp_recv.at[i, j],
                device_id={"tp": (t + i) % TP}, device_id_type=MESH,
            )

    def sends(s):
        for k, d in enumerate(DIRECTIONS):
            if s < N and STEPS[s][d]:
                bulk_copy(s, k, False).start()

    def receives(s):
        for k, d in enumerate(DIRECTIONS):
            if 0 <= s < N and STEPS[s][d]:
                bulk_copy(s, k, True).wait_recv()

    for s in range(AHEAD):
        sends(s)
    for load in loads[3:]:
        load.wait()

    @pl.when(t == 0)
    def _():
        low[t, me] = own_low[0]

    @pl.when(t == 1)
    def _():
        low[t, me] = own_low[1]

    @pl.when(t >= 2)
    def _():
        low[t, me] = own_low[2]

    high2[...] = high[...] * 2.0

    for which, w, start in ((0, rq, 0), (1, rk, Q), (2, rv, Q + KV)):
        rows = own_low[which]
        for j in range(w.shape[2] // KV):
            cols = pl.ds(start + KV * j, KV)
            fresh = w[me, :, pl.ds(KV * j, KV)].astype(jnp.float32) + lax.dot_general(
                rows, high2[:, cols], (((0,), (0,)), ((), ())), preferred_element_type=jnp.float32
            )
            sums[me, :, cols] = jnp.sum(fresh * fresh, axis=0, keepdims=True)
    sums[me, :, pl.ds(COLS, 128)] = jnp.concatenate([norm_in[0] + norm_in[1]] * 2, axis=1)

    def scales():
        total = sums[0, :, pl.ds(0, COLS)]
        for b in range(1, BLOCKS):
            total = total + sums[b, :, pl.ds(0, COLS)]
        scale = jnp.sqrt(total)
        column[...] = scale
        inv[...] = 1.0 / scale
        norms[t] = sums[:, 0, pl.ds(COLS, 128)]
        lane = lax.broadcasted_iota(jnp.int32, (BLOCKS, 128), 1)
        for p in range(2):
            lines[pl.ds(p, BLOCKS, stride=2), :] = jnp.where(lane < 64, norms[2 * p], norms[2 * p + 1])
        norm_out[...] = lines[...].astype(jnp.bfloat16)

    lag = AHEAD + 1
    last_small = len(SMALL_STEPS) - 1 + lag + AHEAD
    done = 0
    for s in range(AHEAD, N + AHEAD):
        receives(s - AHEAD)
        for item in smalls(s - lag - AHEAD):
            small_copy(*item, True).wait_recv()
        sends(s)
        for item in smalls(s - lag):
            small_copy(*item, False).start()
        if s == last_small:
            for i in range(1, TP):
                for copy in tp_copies(t, i):
                    copy.start()
        if s == last_small + TP_WAIT:
            for i in range(1, TP):
                for copy in tp_copies((t + TP - i) % TP, i):
                    copy.wait_recv()
            scales()
        if s > last_small + TP_WAIT:
            while done < BLOCKS and done < 2 * (s - last_small - TP_WAIT):
                for which in range(3):
                    left[which, done] = low[which, done].T
                done += 1
    assert done == BLOCKS
    for i in range(1, TP):
        for copy in tp_copies(t, i):
            copy.wait_send()
    for s in range(len(SMALL_STEPS)):
        for item in smalls(s):
            small_copy(*item, False).wait_send()
    for s in range(N):
        for k, d in enumerate(DIRECTIONS):
            if STEPS[s][d]:
                bulk_copy(s, k, False).wait_send()


def merge_kernel(
    rq, rk, rv, left, high2, inv, column, norm,
    sq, sk, sv, cq, ck, cv, norm_out,
    oq, ok, ov, out_sem, end_sem,
):
    ends = [
        pltpu.make_async_copy(src, dst, end_sem.at[i])
        for i, (src, dst) in enumerate(
            (
                (column.at[:, pl.ds(0, Q)], cq),
                (column.at[:, pl.ds(Q, KV)], ck),
                (column.at[:, pl.ds(Q + KV, KV)], cv),
                (norm, norm_out),
            )
        )
    ]
    for copy in ends:
        copy.start()

    parts = ((rq, 0, oq, sq, 0), (rk, 1, ok, sk, Q), (rv, 2, ov, sv, Q + KV))

    def outs(b):
        return [
            pltpu.make_async_copy(o.at[b], serve.at[pl.ds(b * ROWS, ROWS)], out_sem.at[i, b])
            for i, (_, _, o, serve, _) in enumerate(parts)
        ]

    def one(b, _):
        for w, which, o, _, start in parts:
            rows = left[which, b]
            for j in range(w.shape[2] // KV):
                cols = pl.ds(KV * j, KV)
                every = pl.ds(start + KV * j, KV)
                fresh = w[b, :, cols].astype(jnp.float32) + jnp.dot(
                    rows, high2[:, every], preferred_element_type=jnp.float32
                )
                o[b, :, cols] = (fresh * inv[:, every]).astype(jnp.bfloat16)
        for copy in outs(b):
            copy.start()
        return 0

    lax.fori_loop(0, BLOCKS, one, 0)

    def end(b, _):
        for copy in outs(b):
            copy.wait()
        return 0

    lax.fori_loop(0, BLOCKS, end, 0)
    for copy in ends:
        copy.wait()


def on_device(
    weight_query, low_query, high_query,
    weight_key, low_key, high_key,
    weight_value, low_value, high_value,
    norm_train, norm_step,
):
    f32, bf16 = jnp.float32, jnp.bfloat16
    vmem = pl.BlockSpec(memory_space=pltpu.VMEM)
    hbm = pl.BlockSpec(memory_space=pltpu.HBM)
    dma = pltpu.SemaphoreType.DMA
    inputs = (
        weight_query, weight_key, weight_value, low_query.T, low_key.T, low_value.T, high_query, high_key, high_value,
        norm_train.reshape(1, 64), norm_step.reshape(1, 64),
    )
    gathered = pl.pallas_call(
        gather_kernel,
        name="gather",
        out_shape=(
            pltpu.VMEM((BLOCKS, ROWS, Q), bf16),
            pltpu.VMEM((BLOCKS, ROWS, KV), bf16),
            pltpu.VMEM((BLOCKS, ROWS, KV), bf16),
            pltpu.VMEM((3, BLOCKS, ROWS, RANK), bf16),
            pltpu.VMEM((RANK, COLS), bf16),
            pltpu.VMEM((1, COLS), f32),
            pltpu.VMEM((1, COLS), f32),
            pltpu.VMEM((2 * BLOCKS, 128), bf16),
        ),
        in_specs=[hbm] * 11,
        out_specs=[vmem] * 8,
        scratch_shapes=[
            pltpu.VMEM((3, RANK, ROWS), bf16),
            pltpu.VMEM((RANK, COLS), bf16),
            pltpu.VMEM((2, 1, 64), f32),
            pltpu.VMEM((TP, BLOCKS, RANK, ROWS), bf16),
            pltpu.VMEM((BLOCKS, 1, COLS + 128), f32),
            pltpu.VMEM((TP, BLOCKS, 128), f32),
            pltpu.VMEM((2 * BLOCKS, 128), f32),
            dma((11,)), dma((4, N)), dma((4, N)), dma((3, BLOCKS)), dma((3, BLOCKS)), dma((TP, 2)), dma((TP, 2)),
        ],
        compiler_params=pltpu.CompilerParams(collective_id=0, has_side_effects=True, vmem_limit_bytes=16 << 20),
    )(*(pltpu.with_memory_space_constraint(a, pltpu.HBM) for a in inputs))
    sq, sk, sv, cq, ck, cv, norm = pl.pallas_call(
        merge_kernel,
        name="merge",
        out_shape=(
            pltpu.HBM((BLOCKS * ROWS, Q), bf16),
            pltpu.HBM((BLOCKS * ROWS, KV), bf16),
            pltpu.HBM((BLOCKS * ROWS, KV), bf16),
            pltpu.HBM((1, Q), f32),
            pltpu.HBM((1, KV), f32),
            pltpu.HBM((1, KV), f32),
            pltpu.HBM((2 * BLOCKS, 128), bf16),
        ),
        in_specs=[vmem] * 8,
        out_specs=[hbm] * 7,
        scratch_shapes=[
            pltpu.VMEM((BLOCKS, ROWS, Q), bf16),
            pltpu.VMEM((BLOCKS, ROWS, KV), bf16),
            pltpu.VMEM((BLOCKS, ROWS, KV), bf16),
            dma((3, BLOCKS)),
            dma((4,)),
        ],
        compiler_params=pltpu.CompilerParams(vmem_limit_bytes=24 << 20),
    )(*gathered)
    return sq, sk, sv, cq.reshape(Q), ck.reshape(KV), cv.reshape(KV), norm.reshape(BLOCKS * ROWS)


def solution(mesh):
    rows = P(("unit", "zero"), "tp")
    low = P(("unit", "zero"), None)
    high = P("unit", "tp")
    norm = P(("unit", "zero", "tp"))
    return jax.shard_map(
        on_device,
        mesh=mesh,
        in_specs=(rows, low, high) * 3 + (norm, norm),
        out_specs=(high, high, high, P(("unit", "tp")), P(("unit", "tp")), P(("unit", "tp")), P("unit")),
        check_vma=False,
    )
```

```python
import jax
import jax.numpy as jnp
from jax import lax
from jax.experimental import pallas as pl
from jax.experimental.pallas import tpu as pltpu
from jax.sharding import PartitionSpec as P

MESH = pl.DeviceIdType.MESH
SIDE = 4
BLOCKS = SIDE * SIDE
TP = 4
RANK = 32
ROWS = 256
Q, KV = 1024, 256
COLS = Q + 2 * KV
AHEAD = 4
SMALL_AT = AHEAD
SMALL_LAG = AHEAD
TP_AT = SMALL_AT + 4 * SMALL_LAG
TP_WAIT = 10
DIRECTIONS = ((0, 1), (0, -1), (1, 1), (1, -1))

BULK = [(0, 1, 1), (0, 1, 1), (0, 1, -1), (0, -1, 1), (0, -1, -1), (0, -1, -1)]
BULK = BULK + [(1, s1, s2) for _, s1, s2 in BULK]
BULK_PLACE = [("q", 0), ("q", 1), ("k", 0), ("q", 2), ("v", 0), ("q", 3)]
BULK_PLACE = BULK_PLACE + [("q", 4), ("q", 5), ("k", 1), ("q", 6), ("v", 1), ("q", 7)]
SMALL = [0, 1, 0, 1]
CUT = 768


def children(tree, a, b):
    first, far1, far2 = tree
    out = []
    for axis, sign, here, far, along in (
        (first, 1, a, far1, 0),
        (first, -1, a, far1, 0),
        (1 - first, 1, b, far2, 1),
        (1 - first, -1, b, far2, 1),
    ):
        if along == 0 and b != 0:
            continue
        goes = here == 0 or (here == sign % SIDE and far == sign)
        if goes:
            to = (here + sign) % SIDE
            out.append(((axis, sign), (to, b) if along == 0 else (a, to)))
    return out


def depth(tree, a, b):
    return max((1 + depth(tree, *to) for _, to in children(tree, a, b)), default=0)


def offsets(tree, a, b):
    return (b, a) if tree[0] == 0 else (a, b)


def plan(trees, ahead):
    ready = {d: [] for d in DIRECTIONS}

    def offer(c, a, b, at):
        for d, to in children(trees[c], a, b):
            ready[d].append((at, c, a, b, to))

    for c in range(len(trees)):
        offer(c, 0, 0, -ahead)
    steps = []
    while any(ready.values()):
        s = len(steps)
        now = {}
        for d in DIRECTIONS:
            can = [r for r in ready[d] if r[0] <= s - ahead]
            can.sort(key=lambda r: (-depth(trees[r[1]], *r[4]), r[0], r[1]))
            now[d] = can[:1]
            for r in now[d]:
                ready[d].remove(r)
        for d in DIRECTIONS:
            for _, c, a, b, to in now[d]:
                offer(c, *to, s)
        steps.append({d: [r[1:] for r in now[d]] for d in DIRECTIONS})
    return steps


STEPS = plan(BULK, AHEAD)
N = len(STEPS)


def gather_kernel(
    wq, wk, wv, lq, lk, lv, hq, hk, hv, train, step_in,
    rq, rk, rv, left, high2, inv, column, norm_out,
    own_low, high, norm_in, low, sums, norms, lines,
    load_sem, send_sem, recv_sem, small_send, small_recv, tp_send, tp_recv,
):
    me = lax.axis_index("zero")
    t = lax.axis_index("tp")
    y, x = me // SIDE, me % SIDE

    def block(dy, dx):
        return ((y + SIDE - dy) % SIDE) * SIDE + (x + SIDE - dx) % SIDE

    blk = {(dy, dx): block(dy, dx) for dy in range(SIDE) for dx in range(SIDE)}
    towards = {
        (axis, sign): blk[(0, -sign % SIDE) if axis == 0 else (-sign % SIDE, 0)]
        for axis, sign in DIRECTIONS
    }

    barrier = pltpu.get_barrier_semaphore()
    for d in DIRECTIONS:
        pl.semaphore_signal(barrier, inc=1, device_id={"zero": towards[d]}, device_id_type=MESH)
    for i in range(1, TP):
        pl.semaphore_signal(barrier, inc=1, device_id={"tp": (t + i) % TP}, device_id_type=MESH)

    loads = [
        pltpu.make_async_copy(src, dst, load_sem.at[i])
        for i, (src, dst) in enumerate(
            (
                (wq, rq.at[me]), (wk, rk.at[me]), (wv, rv.at[me]),
                (lq, own_low.at[0]), (lk, own_low.at[1]), (lv, own_low.at[2]),
                (hq, high.at[:, pl.ds(0, Q)]), (hk, high.at[:, pl.ds(Q, KV)]), (hv, high.at[:, pl.ds(Q + KV, KV)]),
                (train, norm_in.at[0]), (step_in, norm_in.at[1]),
            )
        )
    ]
    for load in loads:
        load.start()
    for load in loads[:3]:
        load.wait()
    pl.semaphore_wait(barrier, len(DIRECTIONS) + TP - 1)

    def bulk_ref(c, a, b):
        which, i = BULK_PLACE[c]
        ref = {"q": rq, "k": rk, "v": rv}[which]
        rows = 32 if which == "q" else 128
        return ref.at[blk[offsets(BULK[c], a, b)], pl.ds(rows * i, rows)]

    def bulk_copy(s, k, opposite):
        d = DIRECTIONS[k]
        c, a, b, to = STEPS[s][d][0]
        ref = bulk_ref(c, *(to if opposite else (a, b)))
        return pltpu.make_async_remote_copy(
            src_ref=ref, dst_ref=ref, send_sem=send_sem.at[k, s % AHEAD], recv_sem=recv_sem.at[k, s % (2 * AHEAD)],
            device_id={"zero": towards[d]}, device_id_type=MESH,
        )

    def small_ref(c, where):
        if c < 2:
            return low.at[(t, *where, pl.ds(16 * c, 16))]
        return sums.at[(*where, slice(None), pl.ds(0, CUT) if c == 2 else pl.ds(CUT, COLS + 128 - CUT))]

    def small_copies(stage, received=False):
        for c, first in enumerate(SMALL):
            axis = first if stage < 2 else 1 - first
            for n, sign in enumerate((1, -1)):
                if stage == 1 and (n == 0) != (c % 2 == 0):
                    continue
                behind = 0 if stage % 2 == 0 else 1

                def piece(back):
                    at = (x, y)[axis]
                    at = (at + 2 * SIDE - sign * back) % SIDE
                    if stage < 2:
                        return (y, at) if axis == 0 else (at, x)
                    line = slice(None)
                    if stage == 3:
                        line = pl.ds(2 * n, 2)
                    return (line, at) if axis == 0 else (at, line)

                slot = (0, 2, 3, 5)[stage] + (0 if stage == 1 else n)
                ref = small_ref(c, piece(behind + received))
                yield pltpu.make_async_remote_copy(
                    src_ref=ref, dst_ref=ref, send_sem=small_send.at[c, slot], recv_sem=small_recv.at[c, slot],
                    device_id={"zero": towards[axis, sign]}, device_id_type=MESH,
                )

    def tp_copies(owner, i):
        for j, (src, dst) in enumerate(
            ((low.at[owner], low.at[owner]), (sums.at[:, :, 0, pl.ds(COLS, 128)], norms.at[owner]))
        ):
            yield pltpu.make_async_remote_copy(
                src_ref=src, dst_ref=dst, send_sem=tp_send.at[i - 1, j], recv_sem=tp_recv.at[i - 1, j],
                device_id={"tp": (t + i) % TP}, device_id_type=MESH,
            )

    def sends(s):
        for k, d in enumerate(DIRECTIONS):
            if s < N and STEPS[s][d]:
                if s >= AHEAD:
                    bulk_copy(s - AHEAD, k, False).wait_send()
                bulk_copy(s, k, False).start()

    def receives(s):
        for k, d in enumerate(DIRECTIONS):
            if 0 <= s < N and STEPS[s][d]:
                bulk_copy(s, k, True).wait_recv()

    for s in range(AHEAD):
        sends(s)
    for load in loads[3:]:
        load.wait()

    @pl.when(t == 0)
    def _():
        low[t, y, x] = own_low[0]

    @pl.when(t == 1)
    def _():
        low[t, y, x] = own_low[1]

    @pl.when(t >= 2)
    def _():
        low[t, y, x] = own_low[2]

    high2[...] = high[...] * 2.0

    for which, w, start in ((0, rq, 0), (1, rk, Q), (2, rv, Q + KV)):
        rows = own_low[which]
        for j in range(w.shape[2] // KV):
            cols = pl.ds(start + KV * j, KV)
            fresh = w[me, :, pl.ds(KV * j, KV)].astype(jnp.float32) + lax.dot_general(
                rows, high2[:, cols], (((0,), (0,)), ((), ())), preferred_element_type=jnp.float32
            )
            sums[y, x, :, cols] = jnp.sum(fresh * fresh, axis=0, keepdims=True)
    sums[y, x, :, pl.ds(COLS, 128)] = jnp.concatenate([norm_in[0] + norm_in[1]] * 2, axis=1)

    def scales():
        total = sums[0, 0, :, pl.ds(0, COLS)]
        for b in range(1, BLOCKS):
            total = total + sums[b // SIDE, b % SIDE, :, pl.ds(0, COLS)]
        scale = jnp.sqrt(total)
        column[...] = scale
        inv[...] = 1.0 / scale
        norms[t] = sums[:, :, 0, pl.ds(COLS, 128)]
        lane = lax.broadcasted_iota(jnp.int32, (BLOCKS, 128), 1)
        for p in range(2):
            lines[pl.ds(p, BLOCKS, stride=2), :] = jnp.where(
                lane < 64, norms[2 * p].reshape(BLOCKS, 128), norms[2 * p + 1].reshape(BLOCKS, 128)
            )
        norm_out[...] = lines[...].astype(jnp.bfloat16)

    done = 0
    for s in range(AHEAD, N + AHEAD):
        receives(s - AHEAD)
        for stage in range(4):
            if s == SMALL_AT + (stage + 1) * SMALL_LAG:
                for copy in small_copies(stage, True):
                    copy.wait_recv()
        for stage in range(4):
            if s == SMALL_AT + stage * SMALL_LAG:
                for copy in small_copies(stage):
                    copy.start()
        sends(s)
        if s == TP_AT:
            for i in range(1, TP):
                for copy in tp_copies(t, i):
                    copy.start()
        if s == TP_AT + TP_WAIT:
            for i in range(1, TP):
                for copy in tp_copies((t + TP - i) % TP, i):
                    copy.wait_recv()
            scales()
        if s > TP_AT + TP_WAIT:
            while done < min(BLOCKS, 3 * (s - TP_AT - TP_WAIT)):
                for which in range(3):
                    left[which, done] = low[which, done // SIDE, done % SIDE].T
                done += 1
    assert done == BLOCKS
    for i in range(1, TP):
        for copy in tp_copies(t, i):
            copy.wait_send()
    for stage in range(4):
        for copy in small_copies(stage):
            copy.wait_send()
    for s in range(N - AHEAD, N):
        for k, d in enumerate(DIRECTIONS):
            if STEPS[s][d]:
                bulk_copy(s, k, False).wait_send()


def merge_kernel(
    rq, rk, rv, left, high2, inv, column, norm,
    sq, sk, sv, cq, ck, cv, norm_out,
    oq, ok, ov, out_sem, end_sem,
):
    ends = [
        pltpu.make_async_copy(src, dst, end_sem.at[i])
        for i, (src, dst) in enumerate(
            (
                (column.at[:, pl.ds(0, Q)], cq),
                (column.at[:, pl.ds(Q, KV)], ck),
                (column.at[:, pl.ds(Q + KV, KV)], cv),
                (norm, norm_out),
            )
        )
    ]
    for copy in ends:
        copy.start()

    parts = ((rq, 0, oq, sq, 0), (rk, 1, ok, sk, Q), (rv, 2, ov, sv, Q + KV))

    def one(b, _):
        place = pl.ds(pl.multiple_of(b * ROWS, ROWS), ROWS)
        for i, (w, which, o, serve, start) in enumerate(parts):
            rows = left[which, b]
            for j in range(w.shape[2] // KV):
                cols = pl.ds(KV * j, KV)
                every = pl.ds(start + KV * j, KV)
                fresh = w[b, :, cols].astype(jnp.float32) + jnp.dot(
                    rows, high2[:, every], preferred_element_type=jnp.float32
                )
                o[place, cols] = (fresh * inv[:, every]).astype(jnp.bfloat16)
            pltpu.make_async_copy(o.at[place], serve.at[place], out_sem.at[i]).start()
        return 0

    lax.fori_loop(0, BLOCKS, one, 0)
    for i, (_, _, o, serve, _) in enumerate(parts):
        pltpu.make_async_copy(o, serve, out_sem.at[i]).wait()
    for copy in ends:
        copy.wait()


def on_device(
    weight_query, low_query, high_query,
    weight_key, low_key, high_key,
    weight_value, low_value, high_value,
    norm_train, norm_step,
):
    f32, bf16 = jnp.float32, jnp.bfloat16
    vmem = pl.BlockSpec(memory_space=pltpu.VMEM)
    hbm = pl.BlockSpec(memory_space=pltpu.HBM)
    dma = pltpu.SemaphoreType.DMA
    inputs = (
        weight_query, weight_key, weight_value, low_query.T, low_key.T, low_value.T, high_query, high_key, high_value,
        norm_train.reshape(1, 64), norm_step.reshape(1, 64),
    )
    gathered = pl.pallas_call(
        gather_kernel,
        name="gather",
        out_shape=(
            pltpu.VMEM((BLOCKS, ROWS, Q), bf16),
            pltpu.VMEM((BLOCKS, ROWS, KV), bf16),
            pltpu.VMEM((BLOCKS, ROWS, KV), bf16),
            pltpu.VMEM((3, BLOCKS, ROWS, RANK), bf16),
            pltpu.VMEM((RANK, COLS), bf16),
            pltpu.VMEM((1, COLS), f32),
            pltpu.VMEM((1, COLS), f32),
            pltpu.VMEM((2 * BLOCKS, 128), bf16),
        ),
        in_specs=[hbm] * 11,
        out_specs=[vmem] * 8,
        scratch_shapes=[
            pltpu.VMEM((3, RANK, ROWS), bf16),
            pltpu.VMEM((RANK, COLS), bf16),
            pltpu.VMEM((2, 1, 64), f32),
            pltpu.VMEM((TP, SIDE, SIDE, RANK, ROWS), bf16),
            pltpu.VMEM((SIDE, SIDE, 1, COLS + 128), f32),
            pltpu.VMEM((TP, SIDE, SIDE, 128), f32),
            pltpu.VMEM((2 * BLOCKS, 128), f32),
            dma((11,)), dma((4, AHEAD)), dma((4, 2 * AHEAD)), dma((4, 7)), dma((4, 7)), dma((TP - 1, 2)), dma((TP - 1, 2)),
        ],
        compiler_params=pltpu.CompilerParams(collective_id=0, has_side_effects=True, vmem_limit_bytes=16 << 20),
    )(*(pltpu.with_memory_space_constraint(a, pltpu.HBM) for a in inputs))
    sq, sk, sv, cq, ck, cv, norm = pl.pallas_call(
        merge_kernel,
        name="merge",
        out_shape=(
            pltpu.HBM((BLOCKS * ROWS, Q), bf16),
            pltpu.HBM((BLOCKS * ROWS, KV), bf16),
            pltpu.HBM((BLOCKS * ROWS, KV), bf16),
            pltpu.HBM((1, Q), f32),
            pltpu.HBM((1, KV), f32),
            pltpu.HBM((1, KV), f32),
            pltpu.HBM((2 * BLOCKS, 128), bf16),
        ),
        in_specs=[vmem] * 8,
        out_specs=[hbm] * 7,
        scratch_shapes=[
            pltpu.VMEM((BLOCKS * ROWS, Q), bf16),
            pltpu.VMEM((BLOCKS * ROWS, KV), bf16),
            pltpu.VMEM((BLOCKS * ROWS, KV), bf16),
            dma((3,)),
            dma((4,)),
        ],
        compiler_params=pltpu.CompilerParams(vmem_limit_bytes=24 << 20),
    )(*gathered)
    return sq, sk, sv, cq.reshape(Q), ck.reshape(KV), cv.reshape(KV), norm.reshape(BLOCKS * ROWS)


def solution(mesh):
    rows = P(("unit", "zero"), "tp")
    low = P(("unit", "zero"), None)
    high = P("unit", "tp")
    norm = P(("unit", "zero", "tp"))
    return jax.shard_map(
        on_device,
        mesh=mesh,
        in_specs=(rows, low, high) * 3 + (norm, norm),
        out_specs=(high, high, high, P(("unit", "tp")), P(("unit", "tp")), P(("unit", "tp")), P("unit")),
        check_vma=False,
    )
```

```python
import jax
import jax.numpy as jnp
from jax import lax
from jax.experimental import pallas as pl
from jax.experimental.pallas import tpu as pltpu
from jax.sharding import PartitionSpec as P

MESH = pl.DeviceIdType.MESH
SIDE = 4
BLOCKS = SIDE * SIDE
TP = 4
RANK = 32
PART = RANK // TP
ROWS = 256
HALF = ROWS // 2
Q, KV = 1024, 256
COLS = Q + 2 * KV
AHEAD = 4
SMALL_AT = AHEAD
SMALL_LAG = AHEAD
TP_AT = SMALL_AT + 4 * SMALL_LAG
TP_WAIT = 8
UNITS = 4
DIRECTIONS = ((0, 1), (0, -1), (1, 1), (1, -1))

BULK = [(0, 1, 1), (0, 1, 1), (0, 1, -1), (0, -1, 1), (0, -1, -1), (0, -1, -1)]
BULK = BULK + [(1, s1, s2) for _, s1, s2 in BULK]
BULK_PLACE = [("q", 0), ("q", 1), ("k", 0), ("q", 2), ("v", 0), ("q", 3)]
BULK_PLACE = BULK_PLACE + [("q", 4), ("q", 5), ("k", 1), ("q", 6), ("v", 1), ("q", 7)]
SMALL = [0, 1, 0, 1]
CUT = 768


def children(tree, a, b):
    first, far1, far2 = tree
    out = []
    for axis, sign, here, far, along in (
        (first, 1, a, far1, 0),
        (first, -1, a, far1, 0),
        (1 - first, 1, b, far2, 1),
        (1 - first, -1, b, far2, 1),
    ):
        if along == 0 and b != 0:
            continue
        goes = here == 0 or (here == sign % SIDE and far == sign)
        if goes:
            to = (here + sign) % SIDE
            out.append(((axis, sign), (to, b) if along == 0 else (a, to)))
    return out


def depth(tree, a, b):
    return max((1 + depth(tree, *to) for _, to in children(tree, a, b)), default=0)


def offsets(tree, a, b):
    return (b, a) if tree[0] == 0 else (a, b)


def plan(trees, ahead):
    ready = {d: [] for d in DIRECTIONS}

    def offer(c, a, b, at):
        for d, to in children(trees[c], a, b):
            ready[d].append((at, c, a, b, to))

    for c in range(len(trees)):
        offer(c, 0, 0, -ahead)
    steps = []
    while any(ready.values()):
        s = len(steps)
        now = {}
        for d in DIRECTIONS:
            can = [r for r in ready[d] if r[0] <= s - ahead]
            can.sort(key=lambda r: (r[4][1] != 0, min(2 * r[4][0], 7 - r[4][0]), -depth(trees[r[1]], *r[4]), r[0], r[1]))
            now[d] = can[:1]
            for r in now[d]:
                ready[d].remove(r)
        for d in DIRECTIONS:
            for _, c, a, b, to in now[d]:
                offer(c, *to, s)
        steps.append({d: [r[1:] for r in now[d]] for d in DIRECTIONS})
    return steps


STEPS = plan(BULK, AHEAD)
N = len(STEPS)


def half_blocks(steps, trees):
    arrival = {}
    for s, step in enumerate(steps):
        for sent in step.values():
            for c, _, _, to in sent:
                key = (trees[c][0], *offsets(trees[c], *to))
                arrival[key] = max(arrival.get(key, 0), s)
    for half in range(2):
        arrival[half, 0, 0] = -1
    return sorted((at, *key) for key, at in arrival.items())


LAST = SIDE // 2


def merge_plan():
    todo = [u for u in half_blocks(STEPS, BULK) if u[2:] != (LAST, LAST)]
    out = {}
    for s in range(TP_AT + TP_WAIT + 1, N + AHEAD):
        now = [u for u in todo if u[0] + AHEAD <= s][:UNITS]
        todo = todo[len(now) :]
        out[s] = [u[1:] for u in now]
    assert not todo
    return out


MERGES = merge_plan()


def merge_half(raw, low, high2, inv, out, y, x, half, row):
    rows = pl.ds(pl.multiple_of(half * HALF, HALF), HALF)
    start = 0
    for which, (w, o) in enumerate(zip(raw, out)):
        left = low[:, y, x, which, :, rows].astype(jnp.float32).reshape(RANK, HALF).astype(jnp.bfloat16)
        for j in range(w.shape[2] // KV):
            cols, every = pl.ds(KV * j, KV), pl.ds(start + KV * j, KV)
            fresh = w[y * SIDE + x, rows, cols].astype(jnp.float32) + lax.dot_general(
                left, high2[:, every], (((0,), (0,)), ((), ())), preferred_element_type=jnp.float32
            )
            o[pl.ds(row, HALF), cols] = (fresh * inv[:, every]).astype(jnp.bfloat16)
        start += w.shape[2]


def gather_kernel(
    wq, wk, wv, lq, lk, lv, hq, hk, hv, train, step_in,
    rq, rk, rv, oq, ok, ov, low, high2, inv, column, norm_out,
    own_low, high, norm_in, sums, norms, lines,
    load_sem, send_sem, recv_sem, small_send, small_recv, tp_send, tp_recv,
):
    me = lax.axis_index("zero")
    t = lax.axis_index("tp")
    y, x = me // SIDE, me % SIDE

    def block(dy, dx):
        return ((y + SIDE - dy) % SIDE) * SIDE + (x + SIDE - dx) % SIDE

    blk = {(dy, dx): block(dy, dx) for dy in range(SIDE) for dx in range(SIDE)}
    towards = {
        (axis, sign): blk[(0, -sign % SIDE) if axis == 0 else (-sign % SIDE, 0)]
        for axis, sign in DIRECTIONS
    }

    barrier = pltpu.get_barrier_semaphore()
    for d in DIRECTIONS:
        pl.semaphore_signal(barrier, inc=1, device_id={"zero": towards[d]}, device_id_type=MESH)
    for i in range(1, TP):
        pl.semaphore_signal(barrier, inc=1, device_id={"tp": (t + i) % TP}, device_id_type=MESH)

    part = pl.ds(pl.multiple_of(t * PART, PART), PART)
    loads = [
        pltpu.make_async_copy(src, dst, load_sem.at[i])
        for src, dst, i in (
            (wq, rq.at[me], 0), (wk, rk.at[me], 1), (wv, rv.at[me], 2),
            (lq.at[part], low.at[t, y, x, 0], 3), (lk.at[part], low.at[t, y, x, 1], 3), (lv.at[part], low.at[t, y, x, 2], 3),
            (lq, own_low.at[0], 4), (lk, own_low.at[1], 4), (lv, own_low.at[2], 4),
            (hq, high.at[:, pl.ds(0, Q)], 5), (hk, high.at[:, pl.ds(Q, KV)], 5), (hv, high.at[:, pl.ds(Q + KV, KV)], 5),
            (train, norm_in.at[0], 6), (step_in, norm_in.at[1], 6),
        )
    ]
    for load in loads:
        load.start()
    for load in loads[:3]:
        load.wait()
    pl.semaphore_wait(barrier, len(DIRECTIONS) + TP - 1)

    def bulk_ref(c, a, b):
        which, i = BULK_PLACE[c]
        ref = {"q": rq, "k": rk, "v": rv}[which]
        rows = 32 if which == "q" else 128
        return ref.at[blk[offsets(BULK[c], a, b)], pl.ds(rows * i, rows)]

    def bulk_copy(s, k, opposite):
        d = DIRECTIONS[k]
        c, a, b, to = STEPS[s][d][0]
        ref = bulk_ref(c, *(to if opposite else (a, b)))
        return pltpu.make_async_remote_copy(
            src_ref=ref, dst_ref=ref, send_sem=send_sem.at[k], recv_sem=recv_sem.at[k, s % (2 * AHEAD)],
            device_id={"zero": towards[d]}, device_id_type=MESH,
        )

    def small_ref(c, where):
        if c < 2:
            return low.at[(t, *where, slice(None), slice(None), pl.ds(HALF * c, HALF))]
        return sums.at[(*where, slice(None), pl.ds(0, CUT) if c == 2 else pl.ds(CUT, COLS + 128 - CUT))]

    def small_copies(stage, received=False):
        for c, first in enumerate(SMALL):
            axis = first if stage < 2 else 1 - first
            for n, sign in enumerate((1, -1)):
                if stage == 1 and (n == 0) != (c % 2 == 0):
                    continue
                behind = 0 if stage % 2 == 0 else 1

                def piece(back):
                    at = (x, y)[axis]
                    at = (at + 2 * SIDE - sign * back) % SIDE
                    if stage < 2:
                        return (y, at) if axis == 0 else (at, x)
                    line = slice(None)
                    if stage == 3:
                        line = pl.ds(2 * n, 2)
                    return (line, at) if axis == 0 else (at, line)

                ref = small_ref(c, piece(behind + received))
                yield pltpu.make_async_remote_copy(
                    src_ref=ref, dst_ref=ref, send_sem=small_send.at[c, n], recv_sem=small_recv.at[c, n, stage % 2],
                    device_id={"zero": towards[axis, sign]}, device_id_type=MESH,
                )

    def tp_copies(owner, i):
        for j, (src, dst) in enumerate(
            ((low.at[owner], low.at[owner]), (sums.at[:, :, 0, pl.ds(COLS, 128)], norms.at[owner]))
        ):
            yield pltpu.make_async_remote_copy(
                src_ref=src, dst_ref=dst, send_sem=tp_send.at[j], recv_sem=tp_recv.at[j],
                device_id={"tp": (t + i) % TP}, device_id_type=MESH,
            )

    def tp_waits():
        for j, ref in enumerate((low.at[pl.ds(0, TP - 1)], norms.at[pl.ds(0, TP - 1)])):
            yield pltpu.make_async_remote_copy(
                src_ref=ref, dst_ref=ref, send_sem=tp_send.at[j], recv_sem=tp_recv.at[j],
                device_id={"tp": (t + 1) % TP}, device_id_type=MESH,
            )

    def sends(s):
        for k, d in enumerate(DIRECTIONS):
            if s < N and STEPS[s][d]:
                bulk_copy(s, k, False).start()

    def receives(s):
        for k, d in enumerate(DIRECTIONS):
            if 0 <= s < N and STEPS[s][d]:
                bulk_copy(s, k, True).wait_recv()

    for s in range(AHEAD):
        sends(s)
    for i, ref in ((3, low.at[t, y, x]), (4, own_low), (5, high), (6, norm_in)):
        pltpu.make_async_copy(ref, ref, load_sem.at[i]).wait()

    high2[...] = high[...] * 2.0

    for which, w, start in ((0, rq, 0), (1, rk, Q), (2, rv, Q + KV)):
        rows = own_low[which]
        for j in range(w.shape[2] // KV):
            cols = pl.ds(start + KV * j, KV)
            fresh = w[me, :, pl.ds(KV * j, KV)].astype(jnp.float32) + lax.dot_general(
                rows, high2[:, cols], (((0,), (0,)), ((), ())), preferred_element_type=jnp.float32
            )
            sums[y, x, :, cols] = jnp.sum(fresh * fresh, axis=0, keepdims=True)
    sums[y, x, :, pl.ds(COLS, 128)] = jnp.concatenate([norm_in[0] + norm_in[1]] * 2, axis=1)

    def scales():
        total = sums[0, 0, :, pl.ds(0, COLS)]
        for b in range(1, BLOCKS):
            total = total + sums[b // SIDE, b % SIDE, :, pl.ds(0, COLS)]
        scale = jnp.sqrt(total)
        column[...] = scale
        inv[...] = 1.0 / scale
        norms[t] = sums[:, :, 0, pl.ds(COLS, 128)]
        lane = lax.broadcasted_iota(jnp.int32, (BLOCKS, 128), 1)
        for p in range(2):
            lines[pl.ds(p, BLOCKS, stride=2), :] = jnp.where(
                lane < 64, norms[2 * p].reshape(BLOCKS, 128), norms[2 * p + 1].reshape(BLOCKS, 128)
            )
        norm_out[...] = lines[...].astype(jnp.bfloat16)

    def merges(units):
        code = 0
        for half, dy, dx in reversed(units):
            code = 32 * code + (half * SIDE + dy) * SIDE + dx

        def one(_, code):
            half, dy, dx = code % 32 // BLOCKS, code % BLOCKS // SIDE, code % SIDE
            by, bx = (y + SIDE - dy) % SIDE, (x + SIDE - dx) % SIDE
            row = pl.multiple_of((by * SIDE + bx) * ROWS + half * HALF, HALF)
            merge_half((rq, rk, rv), low, high2, inv, (oq, ok, ov), by, bx, half, row)
            return code // 32

        if units:
            lax.fori_loop(0, len(units), one, jnp.int32(code))

    for s in range(AHEAD, N + AHEAD):
        receives(s - AHEAD)
        for stage in range(4):
            if s == SMALL_AT + (stage + 1) * SMALL_LAG:
                for copy in small_copies(stage, True):
                    copy.wait_recv()
                for copy in small_copies(stage):
                    copy.wait_send()
        for stage in range(4):
            if s == SMALL_AT + stage * SMALL_LAG:
                for copy in small_copies(stage):
                    copy.start()
        sends(s)
        if s == TP_AT:
            for i in range(1, TP):
                for copy in tp_copies(t, i):
                    copy.start()
        if s == TP_AT + TP_WAIT:
            for copy in tp_waits():
                copy.wait_recv()
            scales()
        merges(MERGES.get(s, []))
    for copy in tp_waits():
        copy.wait_send()
    for k in range(len(DIRECTIONS)):
        every = rq.at[pl.ds(0, BLOCKS - 1), pl.ds(0, 2 * N * ROWS // (BLOCKS - 1) // 16)]
        pltpu.make_async_remote_copy(
            src_ref=every, dst_ref=every, send_sem=send_sem.at[k], recv_sem=recv_sem.at[k, 0],
            device_id={"zero": towards[DIRECTIONS[k]]}, device_id_type=MESH,
        ).wait_send()


def merge_kernel(
    rq, rk, rv, oq, ok, ov, low, high2, inv, column, norm,
    sq, sk, sv, cq, ck, cv, norm_out,
    lq, lk, lv, out_sem, end_sem,
):
    me = lax.axis_index("zero")
    y, x = (me // SIDE + LAST) % SIDE, (me + LAST) % SIDE
    last = y * SIDE + x
    outs = ((oq, lq, sq), (ok, lk, sk), (ov, lv, sv))

    def one(i, _):
        b = (last + 1 + i) % BLOCKS
        rows = pl.ds(pl.multiple_of(b * ROWS, ROWS), ROWS)
        for i, (o, _, s) in enumerate(outs):
            pltpu.make_async_copy(o.at[rows], s.at[rows], out_sem.at[i]).start()
        return 0

    lax.fori_loop(0, BLOCKS - 1, one, 0)
    ends = [
        pltpu.make_async_copy(src, dst, end_sem.at[i])
        for i, (src, dst) in enumerate(
            (
                (column.at[:, pl.ds(0, Q)], cq),
                (column.at[:, pl.ds(Q, KV)], ck),
                (column.at[:, pl.ds(Q + KV, KV)], cv),
                (norm, norm_out),
            )
        )
    ]
    for copy in ends:
        copy.start()
    for half in range(2):
        merge_half((rq, rk, rv), low, high2, inv, (lq, lk, lv), y, x, half, half * HALF)
    rows = pl.ds(pl.multiple_of(last * ROWS, ROWS), ROWS)
    for i, (_, o, s) in enumerate(outs):
        pltpu.make_async_copy(o, s.at[rows], out_sem.at[i]).start()
    for i, (o, _, s) in enumerate(outs):
        pltpu.make_async_copy(o, s, out_sem.at[i]).wait()
    for copy in ends:
        copy.wait()


def on_device(
    weight_query, low_query, high_query,
    weight_key, low_key, high_key,
    weight_value, low_value, high_value,
    norm_train, norm_step,
):
    f32, bf16 = jnp.float32, jnp.bfloat16
    vmem = pl.BlockSpec(memory_space=pltpu.VMEM)
    hbm = pl.BlockSpec(memory_space=pltpu.HBM)
    dma = pltpu.SemaphoreType.DMA
    inputs = (
        weight_query, weight_key, weight_value, low_query.T, low_key.T, low_value.T, high_query, high_key, high_value,
        norm_train.reshape(1, 64), norm_step.reshape(1, 64),
    )
    gathered = pl.pallas_call(
        gather_kernel,
        name="gather",
        out_shape=(
            pltpu.VMEM((BLOCKS, ROWS, Q), bf16),
            pltpu.VMEM((BLOCKS, ROWS, KV), bf16),
            pltpu.VMEM((BLOCKS, ROWS, KV), bf16),
            pltpu.VMEM((BLOCKS * ROWS, Q), bf16),
            pltpu.VMEM((BLOCKS * ROWS, KV), bf16),
            pltpu.VMEM((BLOCKS * ROWS, KV), bf16),
            pltpu.VMEM((TP, SIDE, SIDE, 3, PART, ROWS), bf16),
            pltpu.VMEM((RANK, COLS), bf16),
            pltpu.VMEM((1, COLS), f32),
            pltpu.VMEM((1, COLS), f32),
            pltpu.VMEM((2 * BLOCKS, 128), bf16),
        ),
        in_specs=[hbm] * 11,
        out_specs=[vmem] * 11,
        scratch_shapes=[
            pltpu.VMEM((3, RANK, ROWS), bf16),
            pltpu.VMEM((RANK, COLS), bf16),
            pltpu.VMEM((2, 1, 64), f32),
            pltpu.VMEM((SIDE, SIDE, 1, COLS + 128), f32),
            pltpu.VMEM((TP, SIDE, SIDE, 128), f32),
            pltpu.VMEM((2 * BLOCKS, 128), f32),
            dma((7,)), dma((4,)), dma((4, 2 * AHEAD)), dma((4, 2)), dma((4, 2, 2)), dma((2,)), dma((2,)),
        ],
        compiler_params=pltpu.CompilerParams(collective_id=0, has_side_effects=True, vmem_limit_bytes=16 << 20),
    )(*(pltpu.with_memory_space_constraint(a, pltpu.HBM) for a in inputs))
    sq, sk, sv, cq, ck, cv, norm = pl.pallas_call(
        merge_kernel,
        name="merge",
        out_shape=(
            pltpu.HBM((BLOCKS * ROWS, Q), bf16),
            pltpu.HBM((BLOCKS * ROWS, KV), bf16),
            pltpu.HBM((BLOCKS * ROWS, KV), bf16),
            pltpu.HBM((1, Q), f32),
            pltpu.HBM((1, KV), f32),
            pltpu.HBM((1, KV), f32),
            pltpu.HBM((2 * BLOCKS, 128), bf16),
        ),
        in_specs=[vmem] * 11,
        out_specs=[hbm] * 7,
        scratch_shapes=[
            pltpu.VMEM((ROWS, Q), bf16),
            pltpu.VMEM((ROWS, KV), bf16),
            pltpu.VMEM((ROWS, KV), bf16),
            dma((3,)),
            dma((4,)),
        ],
        compiler_params=pltpu.CompilerParams(vmem_limit_bytes=16 << 20),
    )(*gathered)
    return sq, sk, sv, cq.reshape(Q), ck.reshape(KV), cv.reshape(KV), norm.reshape(BLOCKS * ROWS)


def solution(mesh):
    rows = P(("unit", "zero"), "tp")
    low = P(("unit", "zero"), None)
    high = P("unit", "tp")
    norm = P(("unit", "zero", "tp"))
    return jax.shard_map(
        on_device,
        mesh=mesh,
        in_specs=(rows, low, high) * 3 + (norm, norm),
        out_specs=(high, high, high, P(("unit", "tp")), P(("unit", "tp")), P(("unit", "tp")), P("unit")),
        check_vma=False,
    )
```

```python
import jax
import jax.numpy as jnp
from jax import lax
from jax.experimental import pallas as pl
from jax.experimental.pallas import tpu as pltpu
from jax.sharding import PartitionSpec as P

MESH = pl.DeviceIdType.MESH
SIDE = 4
BLOCKS = SIDE * SIDE
TP = 4
RANK = 32
PART = RANK // TP
ROWS = 256
HALF = ROWS // 2
Q, KV = 1024, 256
COLS = Q + 2 * KV
AHEAD = 4
SMALL_LAG = AHEAD
STAGE_AT = tuple(AHEAD + i * SMALL_LAG + (i > 1) for i in range(4))
TP_AT = STAGE_AT[3] + SMALL_LAG
TP_WAIT = 8
UNITS = 4
DIRECTIONS = ((0, 1), (0, -1), (1, 1), (1, -1))

BULK = [(0, 1, 1), (0, 1, 1), (0, 1, -1), (0, -1, 1), (0, -1, -1), (0, -1, -1)]
BULK = BULK + [(1, s1, s2) for _, s1, s2 in BULK]
BULK_PLACE = [("q", 0), ("q", 1), ("k", 0), ("q", 2), ("v", 0), ("q", 3)]
BULK_PLACE = BULK_PLACE + [("q", 4), ("q", 5), ("k", 1), ("q", 6), ("v", 1), ("q", 7)]
SMALL = [0, 1, 0, 1, 0]
CUT = 768


def children(tree, a, b):
    first, far1, far2 = tree
    out = []
    for axis, sign, here, far, along in (
        (first, 1, a, far1, 0),
        (first, -1, a, far1, 0),
        (1 - first, 1, b, far2, 1),
        (1 - first, -1, b, far2, 1),
    ):
        if along == 0 and b != 0:
            continue
        goes = here == 0 or (here == sign % SIDE and far == sign)
        if goes:
            to = (here + sign) % SIDE
            out.append(((axis, sign), (to, b) if along == 0 else (a, to)))
    return out


def depth(tree, a, b):
    return max((1 + depth(tree, *to) for _, to in children(tree, a, b)), default=0)


def offsets(tree, a, b):
    return (b, a) if tree[0] == 0 else (a, b)


def plan(trees, ahead):
    ready = {d: [] for d in DIRECTIONS}

    def offer(c, a, b, at):
        for d, to in children(trees[c], a, b):
            ready[d].append((at, c, a, b, to))

    for c in range(len(trees)):
        offer(c, 0, 0, -ahead)
    steps = []
    while any(ready.values()):
        s = len(steps)
        now = {}
        for d in DIRECTIONS:
            can = [r for r in ready[d] if r[0] <= s - ahead]
            can.sort(key=lambda r: (r[4][1] != 0, min(2 * r[4][0], 7 - r[4][0]), -depth(trees[r[1]], *r[4]), r[0], r[1]))
            now[d] = can[:1]
            for r in now[d]:
                ready[d].remove(r)
        for d in DIRECTIONS:
            for _, c, a, b, to in now[d]:
                offer(c, *to, s)
        steps.append({d: [r[1:] for r in now[d]] for d in DIRECTIONS})
    return steps


STEPS = plan(BULK, AHEAD)
N = len(STEPS)


def half_blocks(steps, trees):
    arrival = {}
    for s, step in enumerate(steps):
        for sent in step.values():
            for c, _, _, to in sent:
                key = (trees[c][0], *offsets(trees[c], *to))
                arrival[key] = max(arrival.get(key, 0), s)
    for half in range(2):
        arrival[half, 0, 0] = -1
    return sorted((at, *key) for key, at in arrival.items())


LAST = SIDE // 2


def merge_plan():
    todo = [u for u in half_blocks(STEPS, BULK) if u[2:] != (LAST, LAST)]
    out = {}
    for s in range(TP_AT + TP_WAIT + 1, N + AHEAD):
        now = [u for u in todo if u[0] + AHEAD <= s][:UNITS]
        todo = todo[len(now) :]
        out[s] = [u[1:] for u in now]
    assert not todo
    return out


MERGES = merge_plan()


def merge_half(raw, low, high2, inv, out, y, x, half, row):
    rows = pl.ds(pl.multiple_of(half * HALF, HALF), HALF)
    start = 0
    for which, (w, o) in enumerate(zip(raw, out)):
        left = low[:, y, x, which, :, rows].astype(jnp.float32).reshape(RANK, HALF).astype(jnp.bfloat16)
        for j in range(w.shape[2] // KV):
            cols, every = pl.ds(KV * j, KV), pl.ds(start + KV * j, KV)
            fresh = w[y * SIDE + x, rows, cols].astype(jnp.float32) + lax.dot_general(
                left, high2[:, every], (((0,), (0,)), ((), ())), preferred_element_type=jnp.float32
            )
            o[pl.ds(row, HALF), cols] = (fresh * inv[:, every]).astype(jnp.bfloat16)
        start += w.shape[2]


def gather_kernel(
    wq, wk, wv, lq, lk, lv, hq, hk, hv, train, step_in,
    rq, rk, rv, oq, ok, ov, low, high2, inv, column, norm_out,
    own_low, high, norm_in, sums, line_sums, norms, lines,
    load_sem, send_sem, recv_sem, small_send, small_recv, tp_send, tp_recv,
):
    me = lax.axis_index("zero")
    t = lax.axis_index("tp")
    y, x = me // SIDE, me % SIDE

    def block(dy, dx):
        return ((y + SIDE - dy) % SIDE) * SIDE + (x + SIDE - dx) % SIDE

    blk = {(dy, dx): block(dy, dx) for dy in range(SIDE) for dx in range(SIDE)}
    towards = {
        (axis, sign): blk[(0, -sign % SIDE) if axis == 0 else (-sign % SIDE, 0)]
        for axis, sign in DIRECTIONS
    }

    barrier = pltpu.get_barrier_semaphore()
    for d in DIRECTIONS:
        pl.semaphore_signal(barrier, inc=1, device_id={"zero": towards[d]}, device_id_type=MESH)
    for i in range(1, TP):
        pl.semaphore_signal(barrier, inc=1, device_id={"tp": (t + i) % TP}, device_id_type=MESH)

    part = pl.ds(pl.multiple_of(t * PART, PART), PART)
    loads = [
        pltpu.make_async_copy(src, dst, load_sem.at[i])
        for src, dst, i in (
            (wq, rq.at[me], 0), (wk, rk.at[me], 1), (wv, rv.at[me], 2),
            (lq.at[part], low.at[t, y, x, 0], 3), (lk.at[part], low.at[t, y, x, 1], 3), (lv.at[part], low.at[t, y, x, 2], 3),
            (lq, own_low.at[0], 4), (lk, own_low.at[1], 4), (lv, own_low.at[2], 4),
            (hq, high.at[:, pl.ds(0, Q)], 5), (hk, high.at[:, pl.ds(Q, KV)], 5), (hv, high.at[:, pl.ds(Q + KV, KV)], 5),
            (train, norm_in.at[0], 6), (step_in, norm_in.at[1], 6),
        )
    ]
    for load in loads:
        load.start()
    for load in loads[:3]:
        load.wait()
    pl.semaphore_wait(barrier, len(DIRECTIONS) + TP - 1)

    def bulk_ref(c, a, b):
        which, i = BULK_PLACE[c]
        ref = {"q": rq, "k": rk, "v": rv}[which]
        rows = 32 if which == "q" else 128
        return ref.at[blk[offsets(BULK[c], a, b)], pl.ds(rows * i, rows)]

    def bulk_copy(s, k, opposite):
        d = DIRECTIONS[k]
        c, a, b, to = STEPS[s][d][0]
        ref = bulk_ref(c, *(to if opposite else (a, b)))
        return pltpu.make_async_remote_copy(
            src_ref=ref, dst_ref=ref, send_sem=send_sem.at[k], recv_sem=recv_sem.at[k, s % (2 * AHEAD)],
            device_id={"zero": towards[d]}, device_id_type=MESH,
        )

    def small_ref(c, where):
        if c < 2:
            return low.at[(t, *where, slice(None), slice(None), pl.ds(HALF * c, HALF))]
        return sums.at[(*where, slice(None), pl.ds(*((0, CUT), (CUT, COLS - CUT), (COLS, 128))[c - 2]))]

    def small_copies(stage, received=False):
        for c, first in enumerate(SMALL):
            axis = first if stage < 2 else 1 - first
            summed = c in (2, 3) and stage >= 2
            for n, sign in enumerate((1, -1)):
                if (stage == 1 or stage == 3 and summed) and (n == 0) != (c % 2 == 0):
                    continue
                at = ((x, y)[axis] + 2 * SIDE - sign * (stage % 2 + received)) % SIDE
                if summed:
                    ref = line_sums.at[c - 2, at]
                else:
                    across = (y, x)[axis] if stage < 2 else slice(None) if stage == 2 else pl.ds(2 * n, 2)
                    ref = small_ref(c, (across, at) if axis == 0 else (at, across))
                yield pltpu.make_async_remote_copy(
                    src_ref=ref, dst_ref=ref, send_sem=small_send.at[c, n], recv_sem=small_recv.at[c, n, stage % 2],
                    device_id={"zero": towards[axis, sign]}, device_id_type=MESH,
                )

    def line_totals():
        for c, here in ((2, y), (3, x)):
            total = small_ref(c, (y, 0) if c == 2 else (0, x))[...]
            for i in range(1, SIDE):
                total = total + small_ref(c, (y, i) if c == 2 else (i, x))[...]
            line_sums[c - 2, here] = total

    def tp_copies(owner, i):
        for j, (src, dst) in enumerate(
            ((low.at[owner], low.at[owner]), (sums.at[:, :, 0, pl.ds(COLS, 128)], norms.at[owner]))
        ):
            yield pltpu.make_async_remote_copy(
                src_ref=src, dst_ref=dst, send_sem=tp_send.at[j], recv_sem=tp_recv.at[j],
                device_id={"tp": (t + i) % TP}, device_id_type=MESH,
            )

    def tp_waits():
        for j, ref in enumerate((low.at[pl.ds(0, TP - 1)], norms.at[pl.ds(0, TP - 1)])):
            yield pltpu.make_async_remote_copy(
                src_ref=ref, dst_ref=ref, send_sem=tp_send.at[j], recv_sem=tp_recv.at[j],
                device_id={"tp": (t + 1) % TP}, device_id_type=MESH,
            )

    def sends(s):
        for k, d in enumerate(DIRECTIONS):
            if s < N and STEPS[s][d]:
                bulk_copy(s, k, False).start()

    def receives(s):
        for k, d in enumerate(DIRECTIONS):
            if 0 <= s < N and STEPS[s][d]:
                bulk_copy(s, k, True).wait_recv()

    for s in range(AHEAD):
        sends(s)
    for i, ref in ((3, low.at[t, y, x]), (4, own_low), (5, high), (6, norm_in)):
        pltpu.make_async_copy(ref, ref, load_sem.at[i]).wait()

    high2[...] = high[...] * 2.0

    for which, w, start in ((0, rq, 0), (1, rk, Q), (2, rv, Q + KV)):
        rows = own_low[which]
        for j in range(w.shape[2] // KV):
            cols = pl.ds(start + KV * j, KV)
            fresh = w[me, :, pl.ds(KV * j, KV)].astype(jnp.float32) + lax.dot_general(
                rows, high2[:, cols], (((0,), (0,)), ((), ())), preferred_element_type=jnp.float32
            )
            sums[y, x, :, cols] = jnp.sum(fresh * fresh, axis=0, keepdims=True)
    sums[y, x, :, pl.ds(COLS, 128)] = jnp.concatenate([norm_in[0] + norm_in[1]] * 2, axis=1)

    def scales():
        for c, start in ((0, 0), (1, CUT)):
            total = line_sums[c, 0]
            for i in range(1, SIDE):
                total = total + line_sums[c, i]
            scale = jnp.sqrt(total)
            column[:, pl.ds(start, CUT)] = scale
            inv[:, pl.ds(start, CUT)] = 1.0 / scale
        norms[t] = sums[:, :, 0, pl.ds(COLS, 128)]
        lane = lax.broadcasted_iota(jnp.int32, (BLOCKS, 128), 1)
        for p in range(2):
            lines[pl.ds(p, BLOCKS, stride=2), :] = jnp.where(
                lane < 64, norms[2 * p].reshape(BLOCKS, 128), norms[2 * p + 1].reshape(BLOCKS, 128)
            )
        norm_out[...] = lines[...].astype(jnp.bfloat16)

    def merges(units):
        code = 0
        for half, dy, dx in reversed(units):
            code = 32 * code + (half * SIDE + dy) * SIDE + dx

        def one(_, code):
            half, dy, dx = code % 32 // BLOCKS, code % BLOCKS // SIDE, code % SIDE
            by, bx = (y + SIDE - dy) % SIDE, (x + SIDE - dx) % SIDE
            row = pl.multiple_of((by * SIDE + bx) * ROWS + half * HALF, HALF)
            merge_half((rq, rk, rv), low, high2, inv, (oq, ok, ov), by, bx, half, row)
            return code // 32

        if units:
            lax.fori_loop(0, len(units), one, jnp.int32(code))

    for s in range(AHEAD, N + AHEAD):
        receives(s - AHEAD)
        for stage in range(4):
            if s == STAGE_AT[stage] + SMALL_LAG:
                for copy in small_copies(stage, True):
                    copy.wait_recv()
                for copy in small_copies(stage):
                    copy.wait_send()
                if stage == 1:
                    line_totals()
        for stage in range(4):
            if s == STAGE_AT[stage]:
                for copy in small_copies(stage):
                    copy.start()
        sends(s)
        if s == TP_AT:
            for i in range(1, TP):
                for copy in tp_copies(t, i):
                    copy.start()
        if s == TP_AT + TP_WAIT:
            for copy in tp_waits():
                copy.wait_recv()
            scales()
        merges(MERGES.get(s, []))
    for copy in tp_waits():
        copy.wait_send()
    for k in range(len(DIRECTIONS)):
        every = rq.at[pl.ds(0, BLOCKS - 1), pl.ds(0, 2 * N * ROWS // (BLOCKS - 1) // 16)]
        pltpu.make_async_remote_copy(
            src_ref=every, dst_ref=every, send_sem=send_sem.at[k], recv_sem=recv_sem.at[k, 0],
            device_id={"zero": towards[DIRECTIONS[k]]}, device_id_type=MESH,
        ).wait_send()


def merge_kernel(
    rq, rk, rv, oq, ok, ov, low, high2, inv, column, norm,
    sq, sk, sv, cq, ck, cv, norm_out,
    lq, lk, lv, out_sem, end_sem,
):
    me = lax.axis_index("zero")
    y, x = (me // SIDE + LAST) % SIDE, (me + LAST) % SIDE
    last = y * SIDE + x
    outs = ((oq, lq, sq), (ok, lk, sk), (ov, lv, sv))

    def one(i, _):
        b = (last + 1 + i) % BLOCKS
        for half in range(2):
            rows = pl.ds(pl.multiple_of(b * ROWS + half * HALF, HALF), HALF)
            for i, (o, _, s) in enumerate(outs):
                pltpu.make_async_copy(o.at[rows], s.at[rows], out_sem.at[i]).start()
        return 0

    lax.fori_loop(0, BLOCKS - 1, one, 0)
    ends = [
        pltpu.make_async_copy(src, dst, end_sem.at[i])
        for i, (src, dst) in enumerate(
            (
                (column.at[:, pl.ds(0, Q)], cq),
                (column.at[:, pl.ds(Q, KV)], ck),
                (column.at[:, pl.ds(Q + KV, KV)], cv),
                (norm, norm_out),
            )
        )
    ]
    for copy in ends:
        copy.start()
    for half in range(2):
        merge_half((rq, rk, rv), low, high2, inv, (lq, lk, lv), y, x, half, half * HALF)
    rows = pl.ds(pl.multiple_of(last * ROWS, ROWS), ROWS)
    for i, (_, o, s) in enumerate(outs):
        pltpu.make_async_copy(o, s.at[rows], out_sem.at[i]).start()
    for i, (o, _, s) in enumerate(outs):
        pltpu.make_async_copy(o, s, out_sem.at[i]).wait()
    for copy in ends:
        copy.wait()


def on_device(
    weight_query, low_query, high_query,
    weight_key, low_key, high_key,
    weight_value, low_value, high_value,
    norm_train, norm_step,
):
    f32, bf16 = jnp.float32, jnp.bfloat16
    vmem = pl.BlockSpec(memory_space=pltpu.VMEM)
    hbm = pl.BlockSpec(memory_space=pltpu.HBM)
    dma = pltpu.SemaphoreType.DMA
    inputs = (
        weight_query, weight_key, weight_value, low_query.T, low_key.T, low_value.T, high_query, high_key, high_value,
        norm_train.reshape(1, 64), norm_step.reshape(1, 64),
    )
    gathered = pl.pallas_call(
        gather_kernel,
        name="gather",
        out_shape=(
            pltpu.VMEM((BLOCKS, ROWS, Q), bf16),
            pltpu.VMEM((BLOCKS, ROWS, KV), bf16),
            pltpu.VMEM((BLOCKS, ROWS, KV), bf16),
            pltpu.VMEM((BLOCKS * ROWS, Q), bf16),
            pltpu.VMEM((BLOCKS * ROWS, KV), bf16),
            pltpu.VMEM((BLOCKS * ROWS, KV), bf16),
            pltpu.VMEM((TP, SIDE, SIDE, 3, PART, ROWS), bf16),
            pltpu.VMEM((RANK, COLS), bf16),
            pltpu.VMEM((1, COLS), f32),
            pltpu.VMEM((1, COLS), f32),
            pltpu.VMEM((2 * BLOCKS, 128), bf16),
        ),
        in_specs=[hbm] * 11,
        out_specs=[vmem] * 11,
        scratch_shapes=[
            pltpu.VMEM((3, RANK, ROWS), bf16),
            pltpu.VMEM((RANK, COLS), bf16),
            pltpu.VMEM((2, 1, 64), f32),
            pltpu.VMEM((SIDE, SIDE, 1, COLS + 128), f32),
            pltpu.VMEM((2, SIDE, 1, CUT), f32),
            pltpu.VMEM((TP, SIDE, SIDE, 128), f32),
            pltpu.VMEM((2 * BLOCKS, 128), f32),
            dma((7,)), dma((4,)), dma((4, 2 * AHEAD)), dma((5, 2)), dma((5, 2, 2)), dma((2,)), dma((2,)),
        ],
        compiler_params=pltpu.CompilerParams(collective_id=0, has_side_effects=True, vmem_limit_bytes=16 << 20),
    )(*(pltpu.with_memory_space_constraint(a, pltpu.HBM) for a in inputs))
    sq, sk, sv, cq, ck, cv, norm = pl.pallas_call(
        merge_kernel,
        name="merge",
        out_shape=(
            pltpu.HBM((BLOCKS * ROWS, Q), bf16),
            pltpu.HBM((BLOCKS * ROWS, KV), bf16),
            pltpu.HBM((BLOCKS * ROWS, KV), bf16),
            pltpu.HBM((1, Q), f32),
            pltpu.HBM((1, KV), f32),
            pltpu.HBM((1, KV), f32),
            pltpu.HBM((2 * BLOCKS, 128), bf16),
        ),
        in_specs=[vmem] * 11,
        out_specs=[hbm] * 7,
        scratch_shapes=[
            pltpu.VMEM((ROWS, Q), bf16),
            pltpu.VMEM((ROWS, KV), bf16),
            pltpu.VMEM((ROWS, KV), bf16),
            dma((3,)),
            dma((4,)),
        ],
        compiler_params=pltpu.CompilerParams(vmem_limit_bytes=16 << 20),
    )(*gathered)
    return sq, sk, sv, cq.reshape(Q), ck.reshape(KV), cv.reshape(KV), norm.reshape(BLOCKS * ROWS)


def solution(mesh):
    rows = P(("unit", "zero"), "tp")
    low = P(("unit", "zero"), None)
    high = P("unit", "tp")
    norm = P(("unit", "zero", "tp"))
    return jax.shard_map(
        on_device,
        mesh=mesh,
        in_specs=(rows, low, high) * 3 + (norm, norm),
        out_specs=(high, high, high, P(("unit", "tp")), P(("unit", "tp")), P(("unit", "tp")), P("unit")),
        check_vma=False,
    )
```
